32 devices in a mesh: ctx: 16 (over z, y, x), fsdp: 2 (over core).
Axes of the slice: x: 2, y: 2, z: 4, core: 2. Of those that a mesh axis runs over, the one named last changes fastest.
Arguments:
- tokens: bfloat16 [2, 2048, 4096], P('fsdp', 'ctx'), may hold values from -6 to 6
- positions: int32 [2, 2048], P('fsdp', 'ctx'), may hold values from 0 to 2047, as said below
- norm_gain: float32 [4096], replicated, may hold values from 0.5 to 1.5
- query_weight: bfloat16 [4096, 2048], P('fsdp'), may hold values from -1 to 1
- key_weight: bfloat16 [4096, 512], P('fsdp'), may hold values from -1 to 1
- value_matrix: bfloat16 [4096, 512], P('fsdp'), may hold values from -0.09375 to 0.09375
Outputs:
- attended: bfloat16 [2, 2048, 2048], P('fsdp', 'ctx')
The draws below stay inside these ranges and needn't reach their ends.
Inputs may be any that keep to these rules, and one draw needn't show every extreme that they name: In each sequence every position from 0 to 2047 appears once, in runs of 64 consecutive rising positions that begin at multiples of 64 in the array.
All inputs are finite; a program needn't handle non-finite values.
Results may differ from the reference program's by a relative error of at most 0.012.
The reference program's roundings to bfloat16 on the way count: a program that leaves them out, or rounds other values in their place, can miss the bound.
Values may be sent and summed in bfloat16 or wider, within the bound.
No kernel may reach another device: no remote copies, remote signals or barrier semaphores. Data moves between devices by JAX's collectives and lax.ppermute only.
A program may use at most 128 MiB of HBM per device.

```python
import jax
import jax.numpy as jnp
from jax import lax

MODEL_WIDTH = 4096
QUERY_HEADS = 16
KEY_VALUE_HEADS = 4
HEAD_SIZE = 128
TOK_DEV = 128
SEQUENCE_COUNT = 2
SEQUENCE_LENGTH = 2048


def shared_weights(key):
    common = jax.random.truncated_normal(jax.random.fold_in(key, 11), -6.0, 6.0, (MODEL_WIDTH, QUERY_HEADS * HEAD_SIZE), jnp.float32) / jnp.sqrt(1.0 * MODEL_WIDTH)
    separate_streams = jax.random.truncated_normal(jax.random.fold_in(key, 12), -6.0, 6.0, (MODEL_WIDTH, KEY_VALUE_HEADS * HEAD_SIZE), jnp.float32) / jnp.sqrt(1.0 * MODEL_WIDTH)
    query_vectors = common
    key_part = separate_streams
    return (jnp.clip(query_vectors, -1.0, 1.0), jnp.clip(key_part, -1.0, 1.0))


def draw_query_weight(key, part):
    return shared_weights(key)[0].astype(jnp.bfloat16)


def draw_key_weight(key, part):
    return shared_weights(key)[1].astype(jnp.bfloat16)


def draw_positions(key, part):
    block_size = TOK_DEV // 2
    block_count = SEQUENCE_LENGTH // block_size
    orders = jax.vmap(lambda sequence: jax.random.permutation(jax.random.fold_in(key, sequence), block_count))(jnp.arange(SEQUENCE_COUNT, dtype=jnp.int32))
    places = orders[:, :, None] * block_size + jnp.arange(block_size, dtype=jnp.int32)[None, None, :]
    return places.reshape(SEQUENCE_COUNT, SEQUENCE_LENGTH).astype(jnp.int32)


def shard_levels(rng, extent, pieces, low, largest):
    level, own = 1.0, jax.random.fold_in(rng, 6)
    for axis_at, blocks in pieces:
        heights = jnp.exp(jax.random.uniform(jax.random.fold_in(own, axis_at), (blocks,), jnp.float32, low / len(pieces), largest / len(pieces)))
        level = level * jnp.repeat(heights, extent[axis_at] // blocks).reshape([-1 if axis == axis_at else 1 for axis in range(len(extent))])
    return level


def gaussian(own_key, dims, scale, most, pieces=(), kind=jnp.bfloat16):
    result = jax.random.normal(own_key, dims, jnp.float32) * scale
    if len(pieces) > 0:
        result = shard_levels(own_key, dims, pieces, -0.22, 0.18) * result
    return jnp.clip(result, min=-most, max=most).astype(kind)


def setup_inputs(seed: int = 0) -> dict:
    key_list = jax.random.split(jax.random.key(seed), 7)
    tokens = gaussian(key_list[0], (SEQUENCE_COUNT, SEQUENCE_LENGTH, MODEL_WIDTH), 1.0, 6.0, ((0, 2), (1, 16)))
    positions = draw_positions(jax.random.fold_in(key_list[6], 71), 0)
    norm_gain = jnp.clip(1.0 + 0.1 * jax.random.normal(key_list[2], (MODEL_WIDTH,), jnp.float32), 0.5, 1.5)
    query_weight = draw_query_weight(jax.random.fold_in(key_list[6], 71), 0)
    key_weight = draw_key_weight(jax.random.fold_in(key_list[6], 71), 0)
    value_matrix = gaussian(key_list[5], (MODEL_WIDTH, KEY_VALUE_HEADS * HEAD_SIZE), MODEL_WIDTH ** -0.5, 0.09375, ((0, 2),))
    return dict(tokens=tokens, positions=positions, norm_gain=norm_gain, query_weight=query_weight, key_weight=key_weight, value_matrix=value_matrix)


EPS = 1e-05
BASE = 500000.0
MASK_FLOOR = -1e+30

def normalize(tokens, norm_gain):
    values = tokens.astype(jnp.float32)
    inverse = lax.rsqrt(lax.optimization_barrier(jnp.mean(values * values, axis=-1, keepdims=True)) + EPS)
    return (values * inverse * norm_gain.astype(jnp.float32)).astype(jnp.bfloat16)

def rope_tables(places, head_dim):
    half_dim = head_dim // 2
    frequency = BASE ** (-(jnp.arange(half_dim, dtype=jnp.float32) * 2.0) / head_dim)
    angles = places.astype(jnp.float32)[:, None] * frequency[None, :]
    return (jnp.cos(angles), jnp.sin(angles))

def apply_rotation(x, cosine_table_rows, sine_table_rows):
    half_dim = x.shape[-1] // 2
    first_half = x[..., :half_dim]
    second_half = x[..., half_dim:]
    cosine_part = cosine_table_rows[:, None, :]
    sine_part = sine_table_rows[:, None, :]
    return jnp.concatenate([first_half * cosine_part - second_half * sine_part, second_half * cosine_part + first_half * sine_part], axis=-1)

def reference(tokens, positions, norm_gain, query_weight, key_weight, value_matrix):
    query_groups = QUERY_HEADS // KEY_VALUE_HEADS
    normed = normalize(tokens, norm_gain).reshape(SEQUENCE_COUNT * SEQUENCE_LENGTH, MODEL_WIDTH)
    query_unrotated = jnp.dot(normed, query_weight, preferred_element_type=jnp.float32)
    key_unrotated = jnp.dot(normed, key_weight, preferred_element_type=jnp.float32)
    value_projected = jnp.dot(normed, value_matrix, preferred_element_type=jnp.float32)
    cosine_table_rows, sine_table_rows = rope_tables(positions.reshape(SEQUENCE_COUNT * SEQUENCE_LENGTH), HEAD_SIZE)
    query_complete = apply_rotation(query_unrotated.reshape(SEQUENCE_COUNT * SEQUENCE_LENGTH, QUERY_HEADS, HEAD_SIZE), cosine_table_rows, sine_table_rows).astype(jnp.bfloat16).reshape(SEQUENCE_COUNT, SEQUENCE_LENGTH, KEY_VALUE_HEADS, query_groups, HEAD_SIZE)
    key_complete = apply_rotation(key_unrotated.reshape(SEQUENCE_COUNT * SEQUENCE_LENGTH, KEY_VALUE_HEADS, HEAD_SIZE), cosine_table_rows, sine_table_rows).astype(jnp.bfloat16).reshape(SEQUENCE_COUNT, SEQUENCE_LENGTH, KEY_VALUE_HEADS, HEAD_SIZE)
    value_complete = value_projected.astype(jnp.bfloat16).reshape(SEQUENCE_COUNT, SEQUENCE_LENGTH, KEY_VALUE_HEADS, HEAD_SIZE)
    block_size = min(512, SEQUENCE_LENGTH)
    block_count = SEQUENCE_LENGTH // block_size

    def one_sequence(inputs):
        query_seq, key_seq, value_seq, seq_places = inputs
        key_float = key_seq.astype(jnp.float32)
        value_float = value_seq.astype(jnp.float32)

        def one_block(block_index):
            begin = (block_index * block_size).astype(jnp.int32)
            query_block = lax.dynamic_slice_in_dim(query_seq, begin, block_size, 0).astype(jnp.float32)
            query_places = lax.dynamic_slice_in_dim(seq_places, begin, block_size, 0)
            scores = jnp.einsum('qhgd,khd->qhgk', query_block, key_float, precision=lax.Precision.HIGHEST) * HEAD_SIZE ** (-0.5)
            allowed = (seq_places[None, :] <= query_places[:, None])[:, None, None, :]
            scores = jnp.where(allowed, scores, MASK_FLOOR)
            maximum = lax.optimization_barrier(jnp.max(scores, axis=-1, keepdims=True))
            weights = jnp.where(allowed, jnp.exp(scores - maximum), 0.0)
            denominator = lax.optimization_barrier(jnp.sum(weights, axis=-1))
            rounded = weights.astype(jnp.bfloat16).astype(jnp.float32)
            mixed = jnp.einsum('qhgk,khd->qhgd', rounded, value_float, precision=lax.Precision.HIGHEST)
            return (mixed / denominator[..., None]).astype(jnp.bfloat16).reshape(block_size, QUERY_HEADS * HEAD_SIZE)
        blocks = lax.map(one_block, jnp.arange(block_count, dtype=jnp.int32))
        return blocks.reshape(SEQUENCE_LENGTH, QUERY_HEADS * HEAD_SIZE)
    return lax.map(one_sequence, (query_complete, key_complete, value_complete, positions))
```

```python
import functools
import math

import jax
import jax.numpy as jnp
from jax import lax
from jax.experimental import pallas as pl
from jax.experimental.pallas import tpu as pltpu
from jax.sharding import PartitionSpec as P

QUERY_HEADS = 16
KEY_VALUE_HEADS = 4
HEAD_SIZE = 128
GROUPS = QUERY_HEADS // KEY_VALUE_HEADS

EPS = 1e-05
BASE = 500000.0
MASK_FLOOR = -1e30
EXP2_SCALE = HEAD_SIZE**-0.5 * math.log2(math.e)
POS_ROWS = 16
POS_SHIFT = 6
MAX_LANE, DEN_LANE, POS_LANE = 0, 32, 64


VMEM = pl.BlockSpec(memory_space=pltpu.VMEM)


def norm_kernel(parts, tokens_ref, gain_ref, *out_refs):
    me = lax.axis_index("fsdp")
    width = tokens_ref.shape[1] // parts
    values = tokens_ref[...].astype(jnp.float32)
    inverse = lax.rsqrt(jnp.mean(values * values, axis=-1, keepdims=True) + EPS)
    for r in range(parts):
        block = lax.rem(me + r, parts)
        columns = pl.ds(pl.multiple_of(block * width, width), width)
        part = tokens_ref[:, columns].astype(jnp.float32)
        out_refs[r][...] = (part * inverse * gain_ref[:, columns]).astype(jnp.bfloat16)


def norm(tokens, gain, parts):
    rows, model = tokens.shape
    tile = rows // 4
    width = model // parts
    return pl.pallas_call(
        functools.partial(norm_kernel, parts),
        grid=(4,),
        in_specs=[
            pl.BlockSpec((tile, model), lambda i: (i, 0)),
            pl.BlockSpec((1, model), lambda i: (0, 0)),
        ],
        out_specs=[pl.BlockSpec((tile, width), lambda i: (i, 0))] * parts,
        out_shape=[jax.ShapeDtypeStruct((rows, width), jnp.bfloat16)] * parts,
        name="norm",
    )(tokens, gain)


def rotate(u, cosine, sine):
    return u * cosine + pltpu.roll(u, HEAD_SIZE // 2, 1) * sine


def total(refs, columns):
    value = refs[0][:, columns]
    for ref in refs[1:]:
        value = value + ref[:, columns]
    return value


def key_value_kernel(parts, members, *refs):
    keys, values = refs[:parts], refs[parts : 2 * parts]
    cosine_ref, sine_ref, places_ref = refs[2 * parts : 2 * parts + 3]
    outs = refs[2 * parts + 3 :]
    me = lax.rem(lax.axis_index("ctx"), members)
    cosine, sine = cosine_ref[...], sine_ref[...]
    places = places_ref[...]
    rows = places.shape[1]
    high = lax.shift_right_logical(places, POS_SHIFT).astype(jnp.float32)
    low = (places & ((1 << POS_SHIFT) - 1)).astype(jnp.float32)
    tail = jnp.broadcast_to(
        jnp.concatenate([high, low], axis=1), (POS_ROWS, 2 * rows)
    ).astype(jnp.bfloat16)
    for k in range(members):
        head = me ^ k
        columns = pl.ds(pl.multiple_of(head * HEAD_SIZE, HEAD_SIZE), HEAD_SIZE)
        out = outs[k]
        out[0:rows, 0:HEAD_SIZE] = rotate(total(keys, columns), cosine, sine).astype(jnp.bfloat16)
        out[0:rows, HEAD_SIZE:] = total(values, columns).astype(jnp.bfloat16)
        out[rows:, :] = tail


def query_kernel(parts, members, *refs):
    queries = refs[:parts]
    cosine_ref, sine_ref = refs[parts : parts + 2]
    outs = refs[parts + 2 :]
    me = lax.rem(lax.axis_index("ctx"), members)
    cosine, sine = cosine_ref[...], sine_ref[...]
    rows = cosine.shape[0]
    for k in range(members):
        for g in range(GROUPS):
            head = (me ^ k) * GROUPS + g
            columns = pl.ds(pl.multiple_of(head * HEAD_SIZE, HEAD_SIZE), HEAD_SIZE)
            outs[k][g * rows : (g + 1) * rows, :] = rotate(
                total(queries, columns), cosine, sine
            ).astype(jnp.bfloat16)


def attend_kernel(members, first, last, *refs):
    queries, chunk_ref = refs[:members], refs[members]
    refs = refs[members + 1 :]
    if not first:
        (stat_in, accum_in), refs = refs[:2], refs[2:]
    if last:
        outs, refs = refs[:members], refs[members:]
    else:
        (stat_out, accum_out), refs = refs[:2], refs[2:]
    key_scratch, value_scratch = refs
    rows = chunk_ref.shape[1] - POS_ROWS
    key_places = []
    for k in range(members):
        key_scratch[k * rows : (k + 1) * rows, :] = chunk_ref[k, 0:rows, 0:HEAD_SIZE]
        value_scratch[k * rows : (k + 1) * rows, :] = chunk_ref[k, 0:rows, HEAD_SIZE:]
        tail = chunk_ref[k, rows:, :].astype(jnp.float32)
        key_places.append(tail[0:1, 0:rows] * (1 << POS_SHIFT) + tail[0:1, rows:])
    all_places = jnp.concatenate(key_places, axis=1)
    keys, values = key_scratch[...], value_scratch[...]
    lane = lax.broadcasted_iota(jnp.int32, (rows, HEAD_SIZE), 1)
    for k in range(members):
        if first:
            places = jnp.transpose(jnp.broadcast_to(key_places[k], (rows, rows)))[:, 0:1]
        for g in range(GROUPS):
            at = (k * GROUPS + g) * rows
            query = queries[k][g * rows : (g + 1) * rows, :]
            scores = lax.dot_general(
                query, keys, (((1,), (1,)), ((), ())), preferred_element_type=jnp.float32
            )
            if not first:
                stat = stat_in[at : at + rows, :]
                places = stat[:, POS_LANE : POS_LANE + 1]
            scores = jnp.where(all_places <= places, scores * EXP2_SCALE, MASK_FLOOR)
            top = jnp.max(scores, axis=-1, keepdims=True)
            if not first:
                old = stat[:, MAX_LANE : MAX_LANE + 1]
                top = jnp.maximum(top, old)
            weights = jnp.exp2(scores - top)
            denominator = jnp.sum(weights, axis=-1, keepdims=True)
            accum = jnp.dot(
                weights.astype(jnp.bfloat16), values, preferred_element_type=jnp.float32
            )
            if not first:
                factor = jnp.exp2(old - top)
                denominator = denominator + factor * stat[:, DEN_LANE : DEN_LANE + 1]
                accum = accum + factor * accum_in[at : at + rows, :]
            if last:
                outs[k][:, g * HEAD_SIZE : (g + 1) * HEAD_SIZE] = (accum / denominator).astype(
                    jnp.bfloat16
                )
            else:
                stat_out[at : at + rows, :] = jnp.where(
                    lane < DEN_LANE, top, jnp.where(lane < POS_LANE, denominator, places)
                )
                accum_out[at : at + rows, :] = accum


def attend(queries, chunk, state, last):
    members = len(queries)
    first = state is None
    rows = chunk.shape[1] - POS_ROWS
    if last:
        out_shape = [jax.ShapeDtypeStruct((rows, GROUPS * HEAD_SIZE), jnp.bfloat16)] * members
    else:
        out_shape = [
            jax.ShapeDtypeStruct((members * GROUPS * rows, HEAD_SIZE), jnp.float32)
        ] * 2
    operands = [*queries, chunk] + ([] if first else list(state))
    keys = members * rows
    scores = members * GROUPS * rows * keys
    return pl.pallas_call(
        functools.partial(attend_kernel, members, first, last),
        in_specs=[VMEM] * len(operands),
        out_specs=[VMEM] * len(out_shape),
        out_shape=out_shape,
        scratch_shapes=[pltpu.VMEM((keys, HEAD_SIZE), jnp.bfloat16)] * 2,
        cost_estimate=pl.CostEstimate(
            flops=4 * scores * HEAD_SIZE, bytes_accessed=1 << 20, transcendentals=scores
        ),
        name="attend",
    )(*operands)


def join_kernel(members, *refs):
    pieces, out = refs[:members], refs[members]
    me = lax.rem(lax.axis_index("ctx"), members)
    width = pieces[0].shape[1]
    for k in range(members):
        columns = pl.ds(pl.multiple_of((me ^ k) * width, width), width)
        out[:, columns] = pieces[k][...]


def on_device(ctx, fsdp, tokens, positions, norm_gain, query_weight, key_weight, value_matrix):
    members = KEY_VALUE_HEADS
    rows = tokens.shape[1]

    def shift(value, by):
        return lax.ppermute(value, "fsdp", [(i, (i + by) % fsdp) for i in range(fsdp)])

    def swap(value, mask):
        return lax.ppermute(value, "ctx", [(i, i ^ mask) for i in range(ctx)])

    normed = norm(tokens[0], norm_gain[None, :], fsdp)
    received = [normed[0]] + [shift(normed[r], r) for r in range(1, fsdp)]

    def project(weight):
        sums = [jnp.dot(part, weight, preferred_element_type=jnp.float32) for part in received]
        return [sums[0]] + [shift(sums[r], fsdp - r) for r in range(1, fsdp)]

    half = HEAD_SIZE // 2
    frequency = BASE ** (-(jnp.arange(half, dtype=jnp.float32) * 2.0) / HEAD_SIZE)
    angles = positions[0].astype(jnp.float32)[:, None] * jnp.concatenate([frequency] * 2)[None, :]
    sign = jnp.where(jnp.arange(HEAD_SIZE) < half, -1.0, 1.0).astype(jnp.float32)
    cosine, sine = jnp.cos(angles), jnp.sin(angles) * sign[None, :]

    keys, values = project(key_weight), project(value_matrix)
    messages = pl.pallas_call(
        functools.partial(key_value_kernel, fsdp, members),
        in_specs=[VMEM] * (2 * fsdp + 3),
        out_specs=[VMEM] * members,
        out_shape=[jax.ShapeDtypeStruct((rows + POS_ROWS, 2 * HEAD_SIZE), jnp.bfloat16)] * members,
        name="key_value",
    )(*keys, *values, cosine, sine, positions)
    chunk = jnp.stack([messages[0]] + [swap(messages[k], k) for k in range(1, members)])

    sums = project(query_weight)
    mine = pl.pallas_call(
        functools.partial(query_kernel, fsdp, members),
        in_specs=[VMEM] * (fsdp + 2),
        out_specs=[VMEM] * members,
        out_shape=[jax.ShapeDtypeStruct((GROUPS * rows, HEAD_SIZE), jnp.bfloat16)] * members,
        name="query",
    )(*sums, cosine, sine)
    queries = [mine[0]] + [swap(mine[k], k) for k in range(1, members)]

    chunks = [chunk]
    bit = ctx // 2
    while bit >= members:
        chunks += [swap(c, bit) for c in chunks]
        bit //= 2
    state = None
    order = sorted(range(len(chunks)), key=lambda c: c != 0)
    for at, c in enumerate(order):
        state = attend(queries, chunks[c], state, at == len(order) - 1)

    pieces = [state[0]] + [swap(state[k], k) for k in range(1, members)]
    out = pl.pallas_call(
        functools.partial(join_kernel, members),
        in_specs=[VMEM] * members,
        out_specs=VMEM,
        out_shape=jax.ShapeDtypeStruct((rows, QUERY_HEADS * HEAD_SIZE), jnp.bfloat16),
        name="join",
    )(*pieces)
    return out[None]


def solution(mesh):
    placed = (
        P("fsdp", "ctx", None),
        P("fsdp", "ctx"),
        P(),
        P("fsdp", None),
        P("fsdp", None),
        P("fsdp", None),
    )
    return jax.shard_map(
        functools.partial(on_device, mesh.shape["ctx"], mesh.shape["fsdp"]),
        mesh=mesh,
        in_specs=placed,
        out_specs=P("fsdp", "ctx", None),
        check_vma=False,
    )
```
